32 devices in a mesh: rows: 8 (over z, x), cols: 4 (over y, core).
Axes of the slice: x: 2, y: 2, z: 4, core: 2. Of those that a mesh axis runs over, the one named last changes fastest.
Arguments:
- leading_scene_data: float32 [2, 1024, 8192], P(None, 'rows', 'cols'), may hold values from -12 to 12, as said below
- trailing_scene_data: float32 [2, 1024, 8192], P(None, 'rows', 'cols'), may hold values from -20 to 20, as said below
- shared_usable_flags: int32 [1024, 8192], P('rows', 'cols'), may hold values 0 or 1
- sweep_of_each_line: int32 [1024], P('rows'), may hold values from 0 to 15, never falling along the last dimension, each value on 1 to 128 neighbouring positions
Outputs:
- deramped: float32 [2, 1024, 8192], P(None, 'rows', 'cols')
- coherence: float32 [1024, 8192], P('rows', 'cols')
The draws below stay inside these ranges and needn't reach their ends.
Inputs may be any that keep to these rules, and one draw needn't show every extreme that they name: `leading_scene_data`: first scene's parts lie in [-12, 12]. `trailing_scene_data`: second scene's parts lie in [-20, 20]; it is the first scene rotated by a smooth phase plus independent noise. `sweep_of_each_line`: burst ids never fall along the rows; each burst holds 1 to 128 rows, one exactly that many.
All inputs are finite; a program needn't handle non-finite values.
Results may differ from the reference program's by a relative error of at most 0.0003.
Values sent between devices are 32-bit elements.
No kernel may reach another device: no remote copies, remote signals or barrier semaphores. Data moves between devices by JAX's collectives and lax.ppermute only.
A program may use at most 64 MiB of HBM per device.

```python
import math
import jax
import jax.numpy as jnp
import numpy as np
from jax import lax

WIN_R = 32
WIN_C = 8
SWEEP_TALLY = 16
SCENE_LINES = 1024
NC = 8192


def scene_primary(key):
    planes = jnp.clip(jax.random.normal(jax.random.fold_in(key, 11), (2, SCENE_LINES, NC), jnp.float32), -6.0, 6.0)
    return planes


def draw_leading_scene_data(key, part):
    return scene_primary(key)


def draw_trailing_scene_data(key, part):
    planes = scene_primary(key)
    speckle = jnp.clip(jax.random.normal(jax.random.fold_in(key, 12), (2, SCENE_LINES, NC), jnp.float32), -6.0, 6.0)
    slopes = jax.random.uniform(jax.random.fold_in(key, 13), (2,), jnp.float32)
    across_slope_term = 2.0 + 2.0 * slopes[0]
    along_slope_term = 1.5 + 1.5 * slopes[1]
    across_coordinate = (jnp.arange(NC, dtype=jnp.float32) + 0.5) / NC
    along_coordinate = (jnp.arange(SCENE_LINES, dtype=jnp.float32) + 0.5) / SCENE_LINES
    planar_angle_fit = across_slope_term * across_coordinate[None, :] + along_slope_term * SWEEP_TALLY * along_coordinate[:, None]
    cos_part = jnp.cos(planar_angle_fit)
    sine_part = jnp.sin(planar_angle_fit)
    real_b = 0.8 * (planes[0] * cos_part + planes[1] * sine_part) + 0.6 * speckle[0]
    imag_b = 0.8 * (planes[1] * cos_part - planes[0] * sine_part) + 0.6 * speckle[1]
    return jnp.stack([real_b, imag_b])


def touch_ends(array, stream_key, smallest, high):
    spot = [jax.random.randint(jax.random.fold_in(stream_key, axis), (), 0, length) for axis, length in enumerate(array.shape)]
    longest = array.shape.index(max(array.shape))
    neighbour = spot[:longest] + [(spot[longest] + 1) % array.shape[longest]] + spot[longest + 1:]
    return array.at[tuple(spot)].set(smallest).at[tuple(neighbour)].set(high)


def profile(count, total, bound, slope):
    weights = [(1 << 20) // math.isqrt(grade ** slope) + 1 for grade in range(2, count + 1)]
    spare, holding = total - bound - (count - 1), [1] * (count - 1)
    while spare > 0:
        candidates = [i for i in range(count - 1) if holding[i] < bound]
        whole, left = sum([weights[i] for i in candidates]), spare
        for i in candidates:
            addition = min(bound - holding[i], max(1, left * weights[i] // whole), spare)
            holding[i] = holding[i] + addition
            spare = spare - addition
    return np.array([bound] + holding)


def ragged(key, count, total, most, skew):
    if count == 2:
        one = jax.random.randint(key, (), max(1, total - most), min(most, total - 1) + 1)
        return jnp.stack([one, total - one])
    tallies = jnp.asarray(profile(count, total, most, skew), jnp.int32)
    couples = (count - 1) // 2
    source_of, taker = tallies[1:1 + 2 * couples:2], tallies[2:2 + 2 * couples:2]
    slack = jnp.minimum(source_of - 1, most - taker)
    passed = jax.random.randint(jax.random.fold_in(key, 1), (couples,), 0, 1 << 20) % (slack + 1)
    tallies = tallies.at[1:1 + 2 * couples:2].set(source_of - passed).at[2:2 + 2 * couples:2].set(taker + passed)
    return tallies[jax.random.permutation(jax.random.fold_in(key, 2), count)]


def setup_inputs(seed: int = 0) -> dict:
    keys = jax.random.split(jax.random.key(seed), 5)
    leading_scene_data = draw_leading_scene_data(jax.random.fold_in(keys[4], 71), 0)
    trailing_scene_data = draw_trailing_scene_data(jax.random.fold_in(keys[4], 71), 0)
    shared_usable_flags = touch_ends((jax.random.randint(keys[2], (SCENE_LINES, NC), 0, 8) < 7).astype(jnp.int32), jax.random.fold_in(keys[2], 1), 0, 1)
    sweep_of_each_line = jnp.searchsorted(jnp.cumsum(ragged(keys[3], SWEEP_TALLY, SCENE_LINES, 2 * SCENE_LINES // SWEEP_TALLY, 1)), jnp.arange(SCENE_LINES), side="right").astype(jnp.int32)
    return {"leading_scene_data": leading_scene_data, "trailing_scene_data": trailing_scene_data, "shared_usable_flags": shared_usable_flags, "sweep_of_each_line": sweep_of_each_line}


largest_value = lax.Precision.HIGHEST

def box_filter(plane):
    zero_value = jnp.zeros((), plane.dtype)
    return lax.reduce_window(plane, zero_value, lax.add, (WIN_R, WIN_C), (1, 1), ((WIN_R // 2, WIN_R // 2 - 1), (WIN_C // 2, WIN_C // 2 - 1)))

def sweep_aggregates(sweep_membership, line_aggregates):
    return jnp.dot(sweep_membership.T, line_aggregates, precision=largest_value)

def solve_ramps(pixel_count, moment_cc, moment_cr, moment_rr, sums):
    ridge_term = 0.001 * pixel_count + 1.0
    diag_col = moment_cc + ridge_term
    diag_row = moment_rr + ridge_term
    determinant = diag_col * diag_row - moment_cr * moment_cr
    base_part = sums[:, 0:2] / (pixel_count + ridge_term)[:, None]
    col_slope = (diag_row[:, None] * sums[:, 2:4] - moment_cr[:, None] * sums[:, 4:6]) / determinant[:, None]
    row_slope = (diag_col[:, None] * sums[:, 4:6] - moment_cr[:, None] * sums[:, 2:4]) / determinant[:, None]
    return jnp.concatenate([base_part, col_slope, row_slope], 1)

def reference(leading_scene_data, trailing_scene_data, shared_usable_flags, sweep_of_each_line):
    weight = shared_usable_flags.astype(jnp.float32)
    real_a = leading_scene_data[0] * weight
    imag_a = leading_scene_data[1] * weight
    real_b = trailing_scene_data[0] * weight
    imag_b = trailing_scene_data[1] * weight
    boxed_real = box_filter(real_a * real_b + imag_a * imag_b)
    boxed_imag = box_filter(imag_a * real_b - real_a * imag_b)
    boxed_pa = box_filter(real_a * real_a + imag_a * imag_a)
    boxed_pb = box_filter(real_b * real_b + imag_b * imag_b)
    normaliser = jnp.sqrt((boxed_pa + 1.0) * (boxed_pb + 1.0))
    coh_real = boxed_real / normaliser
    coh_imag = boxed_imag / normaliser
    coherence = jnp.sqrt(coh_real * coh_real + coh_imag * coh_imag)
    across_coordinate = (jnp.arange(NC, dtype=jnp.float32) + 0.5) * (2.0 / NC) - 1.0
    along_coordinate = (jnp.arange(SCENE_LINES, dtype=jnp.float32) + 0.5) * (2.0 / SCENE_LINES) - 1.0
    sweep_membership = (sweep_of_each_line[:, None] == jnp.arange(SWEEP_TALLY, dtype=jnp.int32)[None, :]).astype(jnp.float32)
    line_usable_tally = lax.optimization_barrier(jnp.sum(weight, 1))
    along_across_moment = lax.optimization_barrier(jnp.sum(weight * across_coordinate[None, :], 1))
    recentered_aggregates = sweep_aggregates(sweep_membership, jnp.stack([line_usable_tally, along_across_moment, along_coordinate * line_usable_tally], 1))
    pixel_count = recentered_aggregates[:, 0]
    floored = jnp.maximum(pixel_count, 1.0)
    middle_across = recentered_aggregates[:, 1] / floored
    middle_along = recentered_aggregates[:, 2] / floored
    along_displacement = along_coordinate - jnp.dot(sweep_membership, middle_along, precision=largest_value)
    across_displacement = across_coordinate[None, :] - jnp.dot(sweep_membership, middle_across, precision=largest_value)[:, None]
    weighted_u = weight * across_displacement
    line_cross_inphase = lax.optimization_barrier(jnp.sum(weight * coh_real, 1))
    line_cross_quadrature = lax.optimization_barrier(jnp.sum(weight * coh_imag, 1))
    along_coordinate_power_two = lax.optimization_barrier(jnp.sum(weighted_u * across_displacement, 1))
    along_first_moment = lax.optimization_barrier(jnp.sum(weighted_u, 1))
    along_weighted_inphase = lax.optimization_barrier(jnp.sum(weighted_u * coh_real, 1))
    along_weighted_quadrature = lax.optimization_barrier(jnp.sum(weighted_u * coh_imag, 1))
    following_picture = sweep_aggregates(sweep_membership, jnp.stack([along_coordinate_power_two, along_displacement * along_first_moment, along_displacement * along_displacement * line_usable_tally, line_cross_inphase, line_cross_quadrature, along_weighted_inphase, along_weighted_quadrature, along_displacement * line_cross_inphase, along_displacement * line_cross_quadrature], 1))
    planar_trends = solve_ramps(pixel_count, following_picture[:, 0], following_picture[:, 1], following_picture[:, 2], following_picture[:, 3:9])
    for_each_line = jnp.dot(sweep_membership, planar_trends, precision=largest_value)
    model_real = for_each_line[:, 0:1] + for_each_line[:, 2:3] * across_displacement + (for_each_line[:, 4] * along_displacement)[:, None]
    model_imag = for_each_line[:, 1:2] + for_each_line[:, 3:4] * across_displacement + (for_each_line[:, 5] * along_displacement)[:, None]
    out_real = coh_real * model_real + coh_imag * model_imag
    out_imag = coh_imag * model_real - coh_real * model_imag
    return (jnp.stack([out_real, out_imag]), coherence)
```

```python
import functools

import jax
import jax.numpy as jnp
from jax import lax
from jax.experimental import pallas as pl
from jax.experimental.pallas import tpu as pltpu
from jax.sharding import PartitionSpec as P

WIN_R = 32
WIN_C = 8
SWEEP_TALLY = 16
HALF = WIN_R // 2
LANES = 128
TABLE_ROWS = 24
TINY = 1.2e-38
EXACT = lax.Precision.HIGHEST
F32 = jnp.float32
BF16 = jnp.bfloat16


def params(mib):
    return pltpu.CompilerParams(vmem_limit_bytes=mib << 20)


def whole():
    return pl.BlockSpec(memory_space=pltpu.VMEM)


def iota(shape, dim):
    return lax.broadcasted_iota(jnp.int32, shape, dim)


def common_phase_removed(ar, ai, br, bi):
    scale = jnp.maximum(jnp.abs(ar), jnp.abs(ai))
    some = scale > TINY
    inverse = 1.0 / jnp.where(some, scale, 1.0)
    xr = ar * inverse
    xi = ai * inverse
    square = jnp.where(some, xr * xr + xi * xi, 1.0)
    inv_root = lax.rsqrt(square)
    ur = jnp.where(some, xr * inv_root, 1.0)
    ui = jnp.where(some, xi * inv_root, 0.0)
    magnitude = jnp.where(some, scale * square * inv_root, 0.0)
    return magnitude, br * ur + bi * ui, bi * ur - br * ui


def masked_phase_removed(lead, trail, flags):
    w = flags.astype(F32)
    return common_phase_removed(lead[0] * w, lead[1] * w, trail[0] * w, trail[1] * w)


def store_strip(lead, trail, flags, out):
    for start in range(0, out.shape[1], 8):
        rows = slice(start, start + 8)
        planes = masked_phase_removed(lead[:, rows], trail[:, rows], flags[rows])
        for p in range(3):
            out[p, rows] = planes[p]


def strip_kernel(lead, trail, flags, out):
    store_strip(lead, trail, flags, out)


def side_kernel(lead, trail, flags, lead_l, trail_l, flags_l, lead_r, trail_r, flags_r, out, left, right):
    store_strip(lead, trail, flags, out)
    lane = iota((1, LANES), 1)
    planes = masked_phase_removed(lead_l[...], trail_l[...], flags_l[...])
    total = jnp.zeros(left.shape, F32)
    for p in range(3):
        place = (lane >= 8 * p) & (lane < 8 * p + WIN_C // 2 - 1)
        total = jnp.where(place, pltpu.roll(planes[p], 8 * p, 1), total)
    left[...] = total
    planes = masked_phase_removed(lead_r[...], trail_r[...], flags_r[...])
    total = jnp.zeros(right.shape, F32)
    for p in range(3):
        from_edge = (lane - 8 * p + LANES) % LANES
        total = jnp.where(from_edge >= LANES - WIN_C // 2, pltpu.roll(planes[p], 8 * p, 1), total)
    right[...] = total


def row_sums(x):
    lanes = x.shape[1]
    x = x + pltpu.roll(x, lanes - 1, 1)
    x = x + pltpu.roll(x, lanes - 2, 1)
    return x + pltpu.roll(x, 4, 1)


def halo_products(packed):
    mag = packed
    br = pltpu.roll(packed, LANES - 8, 1)
    bi = pltpu.roll(packed, LANES - 16, 1)
    return phase_free_products(mag, br, bi)


def phase_free_products(mag, br, bi):
    return mag * br, -(mag * bi), mag * mag, br * br + bi * bi


def split(x):
    high = x.astype(BF16)
    return high, (x - high.astype(F32)).astype(BF16)


def across(cols, total_cols):
    first = (lax.axis_index("cols") * cols).astype(F32)
    return (first + iota((1, cols), 1).astype(F32) + 0.5) * (2.0 / total_cols) - 1.0


def along(shape, dim, rows, total_rows):
    first = (lax.axis_index("rows") * rows).astype(F32)
    return (first + iota(shape, dim).astype(F32) + 0.5) * (2.0 / total_rows) - 1.0


def normalised(sums):
    inverse = lax.rsqrt((sums[2] + 1.0) * (sums[3] + 1.0))
    gr = sums[0] * inverse
    gi = sums[1] * inverse
    return gr, gi


def magnitude_of(gr, gi):
    return jnp.sqrt(gr * gr + gi * gi)


def row_total(x):
    return jnp.sum(x, axis=1, keepdims=True)


def interior_kernel(total_cols, lead, trail, flags, halo, gamma, coh, edge, moments, parts, weight):
    step = pl.program_id(0)
    block = flags.shape[0]
    rows, cols = weight.shape
    here = pl.ds(pl.multiple_of(step * block, block), block)
    low = pl.ds(pl.multiple_of(rows + step * block, block), block)
    u = across(cols, total_cols)
    lane = iota((1, LANES), 1)

    w = flags[...].astype(F32)
    weight[here] = w
    wu = w * u
    moments[here] = jnp.where(
        lane == 0,
        row_total(w),
        jnp.where(lane == 1, row_total(wu), jnp.where(lane == 2, row_total(wu * u), 0.0)),
    )
    outer = halo_products(halo[...])
    ar = lead[0] * w
    ai = lead[1] * w
    br = trail[0] * w
    bi = trail[1] * w
    inner = (
        lambda: ar * br + ai * bi,
        lambda: ai * br - ar * bi,
        lambda: ar * ar + ai * ai,
        lambda: br * br + bi * bi,
    )
    for p in range(4):
        x = jnp.concatenate([inner[p](), outer[p]], 1)
        x = row_sums(x)[:, :cols]
        high, rest = split(x)
        parts[p, here] = high
        parts[p, low] = rest

    @pl.when(step == pl.num_programs(0) - 1)
    def _():
        out_row = iota((rows, 2 * rows), 0)
        in_row = iota((rows, 2 * rows), 1)
        in_row = jnp.where(in_row >= rows, in_row - rows, in_row)
        band = ((in_row >= out_row - HALF) & (in_row < out_row + HALF)).astype(F32).astype(BF16)
        wide = 2 * LANES
        inside = slice(HALF, rows - HALF)
        totals = [jnp.zeros((rows - 2 * HALF, LANES), F32) for _ in range(4)]
        for start in range(0, cols, wide):
            place = slice(start, start + wide)
            sums = [
                jnp.dot(band, parts[p, :, place], preferred_element_type=F32) for p in range(4)
            ]
            for p in range(4):
                edge[p, :HALF, place] = sums[p][:HALF]
                edge[p, HALF:, place] = sums[p][rows - HALF :]
            gr, gi = normalised([s[inside] for s in sums])
            gamma[0, inside, place] = gr
            gamma[1, inside, place] = gi
            coh[inside, place] = magnitude_of(gr, gi)
            w = weight[inside, place]
            wr = w * gr
            wi = w * gi
            uh = u[:, place]
            for q, value in enumerate((wr, wi, wr * uh, wi * uh)):
                totals[q] = totals[q] + value[:, :LANES] + value[:, LANES:]
        found = moments[inside]
        for q in range(4):
            found = jnp.where(lane == 3 + q, row_total(totals[q]), found)
        moments[inside] = found


def edge_kernel(
    sizes, above, below, corner_above, corner_below, edge, flags_top, flags_bottom, moments, sweep, coh_in,
    gamma, coh, table, found, sems,
):
    del coh_in
    total_rows, total_cols = sizes
    cols = edge.shape[2]
    rows = moments.shape[0]
    u = across(cols, total_cols)
    lane = iota((1, LANES), 1)
    out_row = iota((HALF, 2 * HALF), 0)
    in_row = iota((HALF, 2 * HALF), 1)
    in_row = jnp.where(in_row >= HALF, in_row - HALF, in_row)
    masks = (in_row >= out_row, in_row < out_row)
    changes = []
    for side, (strip, corner, flags) in enumerate(
        ((above, corner_above, flags_top), (below, corner_below, flags_bottom))
    ):
        band = masks[side].astype(F32).astype(BF16)
        outer = halo_products(corner[...])
        inner = phase_free_products(strip[0], strip[1], strip[2])
        place = slice(side * HALF, (side + 1) * HALF)
        sums = []
        for p in range(4):
            x = row_sums(jnp.concatenate([inner[p], outer[p]], 1))[:, :cols]
            high, rest = split(x)
            x = jnp.concatenate([high, rest], 0)
            sums.append(edge[p, place] + jnp.dot(band, x, preferred_element_type=F32))
        gr, gi = normalised(sums)
        gamma[0, place] = gr
        gamma[1, place] = gi
        found[place] = magnitude_of(gr, gi)
        first = 0 if side == 0 else rows - HALF
        pltpu.make_async_copy(found.at[place], coh.at[pl.ds(first, HALF)], sems.at[side]).start()
        w = flags[...].astype(F32)
        wr = w * gr
        wi = w * gi
        change = jnp.zeros((HALF, LANES), F32)
        for q, value in enumerate((wr, wi, wr * u, wi * u)):
            change = jnp.where(lane == 3 + q, row_total(value), change)
        changes.append(change)
    full = moments[...] + jnp.concatenate(
        [changes[0], jnp.zeros((rows - 2 * HALF, LANES), F32), changes[1]], 0
    )
    v = along((rows, 1), 0, rows, total_rows)
    by_v = full * v
    full = full + pltpu.roll(by_v, 8, 1) + pltpu.roll(by_v * v, 16, 1)
    member = (iota((LANES, rows), 0) == sweep[...]).astype(F32)
    by_burst = jnp.dot(member, full, precision=EXACT, preferred_element_type=F32)
    table[...] = by_burst.T[: table.shape[0]]
    for side in range(2):
        place = pl.ds(side * HALF, HALF)
        first = 0 if side == 0 else rows - HALF
        pltpu.make_async_copy(found.at[place], coh.at[pl.ds(first, HALF)], sems.at[side]).wait()


def output_kernel(sizes, own, above, below, sweep, gamma, gamma_edge, out, coeffs):
    total_rows, total_cols = sizes
    step = pl.program_id(0)
    last = pl.num_programs(0) - 1
    block, cols = out.shape[1:]
    rows = sweep.shape[1]

    @pl.when(step == 0)
    def _():
        t = own[...] + above[...] + below[...]

        def at(q):
            return t[q : q + 1]

        count, su, suu, sv, suv, svv = at(0), at(1), at(2), at(8), at(9), at(16)
        floored = jnp.maximum(count, 1.0)
        mu = su / floored
        mv = sv / floored
        ridge = 0.001 * count + 1.0
        guu = suu - 2.0 * mu * su + mu * mu * count + ridge
        guv = suv - mu * sv - mv * su + mu * mv * count
        gvv = svv - 2.0 * mv * sv + mv * mv * count + ridge
        determinant = guu * gvv - guv * guv
        terms = []
        for part in range(2):
            h0 = at(3 + part)
            hu = at(5 + part) - mu * h0
            hv = at(11 + part) - mv * h0
            terms.append(h0 / (count + ridge))
            terms.append((gvv * hu - guv * hv) / determinant)
            terms.append((guu * hv - guv * hu) / determinant)
        c = jnp.concatenate(terms + [mu, mv], 0)
        member = (iota((LANES, rows), 0) == sweep[...]).astype(F32)
        c = jnp.dot(c, member, precision=EXACT, preferred_element_type=F32)
        v = along((1, rows), 1, rows, total_rows)
        dv = v - c[7:8]
        base = [c[i : i + 1] + c[i + 2 : i + 3] * dv - c[i + 1 : i + 2] * c[6:7] for i in (0, 3)]
        c = jnp.concatenate([base[0], c[1:2], base[1], c[4:5], jnp.zeros((4, rows), F32)], 0)
        coeffs[...] = c.T

    u = across(cols, total_cols)
    c = coeffs[pl.ds(pl.multiple_of(step * block, block), block)]
    model_r = c[:, 0:1] + c[:, 1:2] * u
    model_i = c[:, 2:3] + c[:, 3:4] * u

    def write(source):
        gr, gi = source[0], source[1]
        out[0] = gr * model_r + gi * model_i
        out[1] = gi * model_r - gr * model_i

    outside = (step == 0) | (step == last)

    @pl.when(outside)
    def _():
        write(gamma_edge)

    @pl.when(jnp.logical_not(outside))
    def _():
        write(gamma)


def neighbours(count):
    forward = [(i, i + 1) for i in range(count - 1)]
    return forward, [(b, a) for a, b in forward]


def over_columns(table):
    count = lax.axis_size("cols")
    if count & (count - 1):
        return lax.psum(table, "cols")
    stride = 1
    while stride < count:
        table = table + lax.ppermute(table, "cols", [(i, i ^ stride) for i in range(count)])
        stride *= 2
    return table


def on_device(leading, trailing, flags, sweep):
    rows, cols = flags.shape
    n_rows, n_cols = lax.axis_size("rows"), lax.axis_size("cols")
    sizes = (rows * n_rows, cols * n_cols)
    last_rows = rows // HALF - 1
    last_cols = cols // LANES - 1
    down, up = neighbours(n_rows)
    right, left = neighbours(n_cols)
    sweep_row = sweep.reshape(1, rows)
    shape = jax.ShapeDtypeStruct

    def row_block(at):
        wide = pl.BlockSpec((2, HALF, cols), lambda i: (0, at, 0))
        return [wide, wide, pl.BlockSpec((HALF, cols), lambda i: (at, 0))]

    def col_block(at):
        tall = pl.BlockSpec((2, rows, LANES), lambda i: (0, 0, at))
        return [tall, tall, pl.BlockSpec((rows, LANES), lambda i: (0, at))]

    scenes = (leading, trailing, flags)
    strip = shape((3, HALF, cols), F32)
    tile = shape((rows, LANES), F32)
    strip_block = pl.BlockSpec((3, HALF, cols), lambda i: (0, 0, 0))
    tile_block = pl.BlockSpec((rows, LANES), lambda i: (0, 0))

    bottom = pl.pallas_call(
        strip_kernel, out_shape=strip, grid=(1,), in_specs=row_block(last_rows), out_specs=strip_block,
        compiler_params=params(8), name="bottom_strip",
    )(*scenes)
    above = lax.ppermute(bottom, "rows", down)
    top, first_cols, final_cols = pl.pallas_call(
        side_kernel, out_shape=(strip, tile, tile), grid=(1,),
        in_specs=row_block(0) + col_block(0) + col_block(last_cols),
        out_specs=(strip_block, tile_block, tile_block), compiler_params=params(8), name="top_and_sides",
    )(*scenes, *scenes, *scenes)
    below = lax.ppermute(top, "rows", up)
    halo = lax.ppermute(final_cols, "cols", right) + lax.ppermute(first_cols, "cols", left)
    corner_above = lax.ppermute(halo[rows - HALF :], "rows", down)
    corner_below = lax.ppermute(halo[:HALF], "rows", up)

    steps = rows // HALF
    gamma, coh, edge, moments = pl.pallas_call(
        functools.partial(interior_kernel, sizes[1]),
        out_shape=(
            shape((2, rows, cols), F32), shape((rows, cols), F32), shape((4, 2 * HALF, cols), F32), tile,
        ),
        grid=(steps,),
        in_specs=[
            pl.BlockSpec((2, HALF, cols), lambda i: (0, i, 0)),
            pl.BlockSpec((2, HALF, cols), lambda i: (0, i, 0)),
            pl.BlockSpec((HALF, cols), lambda i: (i, 0)),
            pl.BlockSpec((HALF, LANES), lambda i: (i, 0)),
        ],
        out_specs=(
            pl.BlockSpec((2, rows, cols), lambda i: (0, 0, 0)),
            pl.BlockSpec((rows, cols), lambda i: (0, 0)),
            pl.BlockSpec((4, 2 * HALF, cols), lambda i: (0, 0, 0)),
            tile_block,
        ),
        scratch_shapes=[pltpu.VMEM((4, 2 * rows, cols), BF16), pltpu.VMEM((rows, cols), F32)],
        compiler_params=params(24), name="interior",
        cost_estimate=pl.CostEstimate(flops=6_000_000_000, bytes_accessed=9 << 20, transcendentals=0),
    )(*scenes, halo)

    flag_row = [pl.BlockSpec((HALF, cols), lambda i: (0, 0)), pl.BlockSpec((HALF, cols), lambda i: (last_rows, 0))]
    one = lambda *block: pl.BlockSpec(block, lambda i: (0,) * len(block))
    gamma_edge, coh, table = pl.pallas_call(
        functools.partial(edge_kernel, sizes),
        out_shape=(
            shape((2, 2 * HALF, cols), F32), shape((rows, cols), F32), shape((TABLE_ROWS, LANES), F32),
        ),
        grid=(1,),
        in_specs=[
            strip_block, strip_block, one(HALF, LANES), one(HALF, LANES), one(4, 2 * HALF, cols),
            *flag_row, tile_block, one(1, rows), pl.BlockSpec(memory_space=pl.ANY),
        ],
        out_specs=(one(2, 2 * HALF, cols), pl.BlockSpec(memory_space=pl.ANY), one(TABLE_ROWS, LANES)),
        input_output_aliases={9: 1},
        scratch_shapes=[pltpu.VMEM((2 * HALF, cols), F32), pltpu.SemaphoreType.DMA((2,))],
        compiler_params=params(12), name="edges",
    )(above, below, corner_above, corner_below, edge, flags, flags, moments, sweep_row, coh)

    longest = 2 * sizes[0] // SWEEP_TALLY
    if longest - 1 <= rows:
        own = over_columns(table)
        from_above = lax.ppermute(own, "rows", down)
        from_below = lax.ppermute(own, "rows", up)
    else:
        own = lax.psum(table, ("rows", "cols"))
        from_above = from_below = jnp.zeros_like(own)

    deramped = pl.pallas_call(
        functools.partial(output_kernel, sizes),
        out_shape=shape((2, rows, cols), F32),
        grid=(steps,),
        in_specs=[
            one(TABLE_ROWS, LANES), one(TABLE_ROWS, LANES), one(TABLE_ROWS, LANES), one(1, rows),
            pl.BlockSpec((2, HALF, cols), lambda i: (0, i, 0)),
            pl.BlockSpec((2, HALF, cols), lambda i: (0, jnp.where(i == 0, 0, 1), 0)),
        ],
        out_specs=pl.BlockSpec((2, HALF, cols), lambda i: (0, i, 0)),
        scratch_shapes=[pltpu.VMEM((rows, 8), F32)],
        compiler_params=params(12), name="model",
    )(own, from_above, from_below, sweep_row, gamma, gamma_edge)
    return deramped, coh


def solution(mesh):
    return jax.shard_map(
        on_device,
        mesh=mesh,
        in_specs=(P(None, "rows", "cols"), P(None, "rows", "cols"), P("rows", "cols"), P("rows")),
        out_specs=(P(None, "rows", "cols"), P("rows", "cols")),
        check_vma=False,
    )
```
